32 devices in a mesh: grp: 4 (over y, x), section: 2 (over core), row: 4 (over z).
Axes of the slice: x: 2, y: 2, z: 4, core: 2. Of those that a mesh axis runs over, the one named last changes fastest.
Arguments:
- matrices: float32 [4, 8192, 8192], P('grp', 'row', 'section'), parts along dimension 0, may hold values from -57 to 57, as said below
Outputs:
- reduced: float32 [4, 8192, 8192], P('grp', 'row', 'section'), parts along dimension 0
The draws below stay inside these ranges and needn't reach their ends.
There are 4 independent parts, one for each index of `grp`. The reference program is written for one: setup_inputs(seed, part) draws one part's arguments, and reference() takes and returns one part's arrays. A program takes and returns all parts, laid end to end along the dimension named above; each array names one. Nothing has to cross between parts.
Inputs may be any that keep to these rules, and one draw needn't show every extreme that they name: `matrices`: each matrix is exactly symmetric.
All inputs are finite; a program needn't handle non-finite values.
Results may differ from the reference program's by a relative error of at most 0.00023.
Values sent between devices are 32-bit elements; how exact they have to be, the bound alone decides.
No kernel may reach another device: no remote copies, remote signals or barrier semaphores. Data moves between devices by JAX's collectives and lax.ppermute only.
A program may use at most 128 MiB of HBM per device.

```python
import jax
import jax.numpy as jnp
from jax import lax

N = 8192
NB = 8
MB = 1


def draw_matrices(key, part):
    normal_draw = jax.random.truncated_normal(key, -4.0, 4.0, (MB, N, N), jnp.float32)
    symmetric = (normal_draw + jnp.swapaxes(normal_draw, 1, 2)) * 0.7071
    return symmetric


def setup_inputs(seed: int = 0, part: int = 0) -> dict:
    streams_of = jax.random.split(jax.random.key(seed), 2)
    part_keys = jax.random.split(jax.random.fold_in(streams_of[1], part), 2)
    matrices = draw_matrices(jax.random.fold_in(jax.random.fold_in(streams_of[1], part), 71), part)
    return {"matrices": matrices}


highest = lax.Precision.HIGHEST

def reference(matrices):
    count = matrices.shape[0]
    order = matrices.shape[1]
    positions = jnp.arange(order, dtype=jnp.int32)
    lefts = jnp.zeros((count, NB, order), jnp.float32)
    rights = jnp.zeros((count, NB, order), jnp.float32)
    for column in range(NB):
        current = matrices[:, :, column]
        current = current - jnp.einsum('mkn,mk->mn', lefts, rights[:, :, column], precision=highest)
        current = current - jnp.einsum('mkn,mk->mn', rights, lefts[:, :, column], precision=highest)
        below = jnp.where(positions[None, :] > column, current, 0.0)
        length = jnp.sqrt(lax.optimization_barrier(jnp.sum(below * below, axis=1)))
        reflector = below + jnp.where(positions[None, :] == column + 1, length[:, None], 0.0)
        scaling = 2.0 / (lax.optimization_barrier(jnp.sum(reflector * reflector, axis=1)) + 1e-06)
        image = jnp.einsum('mij,mj->mi', matrices, reflector, precision=highest)
        right_dots = jnp.einsum('mkn,mn->mk', rights, reflector, precision=highest)
        left_dots = jnp.einsum('mkn,mn->mk', lefts, reflector, precision=highest)
        image = image - jnp.einsum('mkn,mk->mn', lefts, right_dots, precision=highest)
        image = image - jnp.einsum('mkn,mk->mn', rights, left_dots, precision=highest)
        corrected = scaling[:, None] * image
        inner = lax.optimization_barrier(jnp.sum(corrected * reflector, axis=1))
        partner = corrected - (0.5 * scaling * inner)[:, None] * reflector
        lefts = lefts.at[:, column, :].set(reflector)
        rights = rights.at[:, column, :].set(partner)
    reduced = matrices - jnp.einsum('mki,mkj->mij', lefts, rights, precision=highest)
    reduced = reduced - jnp.einsum('mki,mkj->mij', rights, lefts, precision=highest)
    return reduced
```

```python
import functools

import jax
import jax.numpy as jnp
from jax import lax
from jax.experimental import pallas as pl
from jax.experimental.pallas import tpu as pltpu
from jax.sharding import PartitionSpec as P

NB = 8
LANES = 128
SUBLANES = 8
MIB = 1 << 20

VMEM = pltpu.VMEM
f32 = jnp.float32
bf16 = jnp.bfloat16


def call(body, outs, args, scratch=(), flops=0, moved=0, limit=15 * MIB, pinned=(), name=None):
    specs = []
    operands = []
    for index, arg in enumerate(args):
        if index in pinned:
            arg = pltpu.with_memory_space_constraint(arg, VMEM)
        specs.append(pl.BlockSpec(memory_space=VMEM))
        operands.append(arg)
    return pl.pallas_call(
        body,
        out_shape=outs,
        in_specs=specs,
        out_specs=jax.tree.map(lambda _: pl.BlockSpec(memory_space=VMEM), outs),
        scratch_shapes=list(scratch),
        compiler_params=pltpu.CompilerParams(vmem_limit_bytes=limit),
        cost_estimate=pl.CostEstimate(flops=flops, bytes_accessed=moved, transcendentals=0),
        name=name,
    )(*operands)


def out(*shape):
    return jax.ShapeDtypeStruct(shape, f32)


def load_body(src, dst, sems, *, pieces):
    rows = src.shape[0] // pieces
    copies = []
    for k in range(pieces):
        part = pl.ds(k * rows, rows)
        copies.append(pltpu.make_async_copy(src.at[part], dst.at[part], sems.at[k]))
    for copy in copies:
        copy.start()
    for copy in copies:
        copy.wait()


def load(block):
    pieces = 8
    return pl.pallas_call(
        functools.partial(load_body, pieces=pieces),
        out_shape=VMEM(block.shape, f32),
        in_specs=[pl.BlockSpec(memory_space=pl.ANY)],
        out_specs=pl.BlockSpec(memory_space=VMEM),
        scratch_shapes=[pltpu.SemaphoreType.DMA((pieces,))],
        compiler_params=pltpu.CompilerParams(vmem_limit_bytes=15 * MIB),
        cost_estimate=pl.CostEstimate(
            flops=4 * 10**8, bytes_accessed=2 * block.size * 4, transcendentals=0
        ),
        name="load",
    )(pltpu.with_memory_space_constraint(block, pltpu.HBM))


def panel_body(src, dst, tall, sem, *, tiles):
    copy = pltpu.make_async_copy(src.at[:, pl.ds(0, LANES)], tall, sem)
    copy.start()
    copy.wait()
    for t in range(tiles):
        turned = tall[pl.ds(t * LANES, LANES), :].T
        dst[pl.ds(t, NB, stride=tiles), :] = turned[:NB, :]


def panel(block):
    height = block.shape[0]
    tiles = height // LANES
    return pl.pallas_call(
        functools.partial(panel_body, tiles=tiles),
        out_shape=out(NB * tiles, LANES),
        in_specs=[pl.BlockSpec(memory_space=pl.ANY)],
        out_specs=pl.BlockSpec(memory_space=VMEM),
        scratch_shapes=[VMEM((height, LANES), f32), pltpu.SemaphoreType.DMA],
        compiler_params=pltpu.CompilerParams(vmem_limit_bytes=2 * MIB),
        cost_estimate=pl.CostEstimate(flops=10**7, bytes_accessed=2 * MIB, transcendentals=0),
        name="panel",
    )(pltpu.with_memory_space_constraint(block, pltpu.HBM))


def gather_panel_body(*refs, count, sections, tiles):
    dst = refs[-1]
    row = lax.axis_index("row")
    section = lax.axis_index("section")
    own = refs[:count]
    other = refs[count:-1]
    total = tiles * count
    for k in range(count):
        place = lax.rem(row + k, count) * tiles
        for column in range(NB):
            part = pl.ds(column * tiles, tiles)
            value = own[k][part, :]
            if sections == 2:
                value = jnp.where(section == 0, value, other[k][part, :])
            dst[pl.ds(pl.multiple_of(column * total + place, SUBLANES), tiles), :] = value


def total_of(value):
    return jnp.sum(jnp.sum(value, axis=0, keepdims=True), axis=1, keepdims=True)


def place_of(shape):
    return lax.broadcasted_iota(jnp.int32, shape, 0) * LANES + lax.broadcasted_iota(
        jnp.int32, shape, 1
    )


def reflect(current, column):
    place = place_of(current.shape)
    rest = jnp.where(place > column + 1, current, 0.0)
    tail = total_of(rest * rest)
    head = current[0:1, column + 1 : column + 2]
    length = jnp.sqrt(tail + head * head)
    head = head + length
    reflector = jnp.where(place == column + 1, head, rest)
    scaling = 2.0 / (tail + head * head + 1e-06)
    return reflector, scaling, head


def multiply(block, vector, part, wide, *, breadth):
    height = block.shape[0]
    pieces = breadth // LANES
    start = lax.axis_index("section") * pieces
    entries = [vector[pl.ds(start + c, SUBLANES, stride=0), :] for c in range(pieces)]

    def turn(t):
        turned = wide[...].T
        part[pl.ds(t, 1), :] = jnp.sum(turned, axis=0, keepdims=True)

    def step(t, carry):
        @pl.when(t > 0)
        def _():
            turn(t - 1)

        for g in range(LANES // SUBLANES):
            rows = pl.ds(pl.multiple_of(t * LANES + g * SUBLANES, SUBLANES), SUBLANES)
            sums = [None, None]
            for c in range(pieces):
                term = block[rows, pl.ds(c * LANES, LANES)] * entries[c]
                sums[c % 2] = term if sums[c % 2] is None else sums[c % 2] + term
            wide[pl.ds(g * SUBLANES, SUBLANES), :] = sums[0] + sums[1]
        return carry

    lax.fori_loop(0, height // LANES, step, 0)
    turn(height // LANES - 1)


def first_body(panel_ref, block, reflector_ref, facts_ref, part, wide, *, breadth):
    rows = reflector_ref.shape[0]
    reflector, scaling, head = reflect(panel_ref[pl.ds(0, rows), :], 0)
    reflector_ref[...] = reflector
    facts_ref[pl.ds(0, 1), :] = jnp.broadcast_to(scaling, (1, LANES))
    facts_ref[pl.ds(1, 1), :] = jnp.broadcast_to(head, (1, LANES))
    multiply(block, reflector_ref, part, wide, breadth=breadth)


def finish_image(pieces, offset, reflector, facts, image_ref):
    count = len(pieces)
    row = lax.axis_index("row")
    for k, piece in enumerate(pieces):
        tiles = piece.shape[0]
        place = lax.rem(row + k, count) * tiles
        image_ref[pl.ds(pl.multiple_of(place, SUBLANES), tiles), :] = piece[...]
    image = image_ref[...]
    if offset is not None:
        image = image - offset[...]
    scaling = facts[0:1, 0:1]
    corrected = scaling * image
    inner = total_of(corrected * reflector)
    return corrected - (0.5 * scaling * inner) * reflector


def step_body(*refs, column, count, breadth):
    pieces = refs[:count]
    refs = refs[count:]
    if column > 1:
        offset, *refs = refs
    else:
        offset = None
    base, old, facts, block, partner_ref, reflector_ref, facts_ref, part, image, wide = refs
    before = old[...]
    partner = finish_image(pieces, offset, before, facts, image)
    partner_ref[...] = partner
    if column == 1:
        base_value = base[pl.ds(old.shape[0], old.shape[0]), :]
    else:
        base_value = base[...]
    current = base_value - before * partner[0:1, column : column + 1] - partner * facts[1:2, 0:1]
    reflector, scaling, head = reflect(current, column)
    reflector_ref[...] = reflector
    facts_ref[pl.ds(0, 1), :] = jnp.broadcast_to(scaling, (1, LANES))
    facts_ref[pl.ds(1, 1), :] = jnp.broadcast_to(head, (1, LANES))
    multiply(block, reflector_ref, part, wide, breadth=breadth)


def between_body(*refs, column):
    lefts = refs[:column]
    rights = refs[column : 2 * column]
    panel_ref, new, offset_ref = refs[2 * column : 2 * column + 3]
    reflector = new[...]
    rows = reflector.shape[0]
    offset = None
    for left, right in zip(lefts, rights):
        left = left[...]
        right = right[...]
        term = left * total_of(right * reflector) + right * total_of(left * reflector)
        offset = term if offset is None else offset + term
    offset_ref[...] = offset
    after = column + 1
    if after < NB:
        base_ref = refs[-1]
        base = panel_ref[pl.ds(after * rows, rows), :]
        for left, right in zip(lefts, rights):
            left = left[...]
            right = right[...]
            base = base - left * right[0:1, after : after + 1]
            base = base - right * left[0:1, after : after + 1]
        base_ref[...] = base


def add_body(a, b, c):
    c[...] = a[...] + b[...]


def split(value):
    high = value.astype(bf16).astype(f32)
    rest = value - high
    middle = rest.astype(bf16).astype(f32)
    low = (rest - middle).astype(bf16).astype(f32)
    return high, middle, low


def last_body(*refs, count, breadth, slots, tall):
    pieces = refs[:count]
    refs = refs[count:]
    lefts = refs[:NB]
    rights = refs[NB : 2 * NB - 1]
    offset, facts, block, dst, image, stack, right_side, left_side, buffer, sems = refs[2 * NB - 1 :]
    total = image.shape[0]
    height = block.shape[0]
    last = lefts[-1][...]
    partner = finish_image(pieces, offset, last, facts, image)
    for k in range(NB):
        stack[pl.ds(k * total, total), :] = lefts[k][...]
        stack[pl.ds((NB + k) * total, total), :] = partner if k == NB - 1 else rights[k][...]
        stack[pl.ds((2 * NB + k) * total, total), :] = lefts[k][...]
    col_start = lax.axis_index("section") * (breadth // LANES)
    row_start = lax.axis_index("row") * (height // LANES)
    pair = 2 * NB

    for c in range(breadth // LANES):
        rows = stack[pl.ds(NB * total + col_start + c, pair, stride=total), :]
        high, middle, low = split(rows)
        group = jnp.concatenate([high, middle, high, middle, low, high, high * 0.0, high * 0.0], 0)
        right_side[:, pl.ds(c * LANES, LANES)] = group.astype(bf16)

    turns = tall // LANES
    steps = height // tall

    def copy_out(step, slot):
        return pltpu.make_async_copy(
            buffer.at[slot], dst.at[pl.ds(pl.multiple_of(step * tall, tall), tall)], sems.at[slot]
        )

    def step(t, carry):
        slot = lax.rem(t, slots)
        for u in range(turns):
            rows = stack[pl.ds(row_start + t * turns + u, pair, stride=total), :]
            high, middle, low = split(rows)
            group = jnp.concatenate(
                [high, high, middle, middle, high, low, high * 0.0, high * 0.0], 0
            )
            left_side[pl.ds(u * LANES, LANES), :] = group.T.astype(bf16)

        @pl.when(t >= slots)
        def _():
            copy_out(t - slots, slot).wait()

        rows = pl.ds(pl.multiple_of(t * tall, tall), tall)
        wide = 512 if breadth % 512 == 0 else LANES
        for c in range(breadth // wide):
            cols = pl.ds(c * wide, wide)
            change = jnp.dot(left_side[...], right_side[:, cols], preferred_element_type=f32)
            buffer[slot, :, cols] = block[rows, cols] - change
        copy_out(t, slot).start()
        return carry

    lax.fori_loop(0, steps, step, 0)
    for t in range(max(0, steps - slots), steps):
        copy_out(t, t % slots).wait()


def turn_by(axis, size, shift):
    return [(i, (i + shift) % size) for i in range(size)]


def local(matrices):
    height, breadth = matrices.shape[1:]
    count = lax.axis_size("row")
    sections = lax.axis_size("section")
    total = count * height // LANES
    tiles = height // LANES
    direct = count <= 4 and sections == 2
    block = matrices.reshape(height, breadth)

    def rows_of(value):
        got = {}
        for k in range(1, count):
            got[k] = lax.ppermute(value, "row", turn_by("row", count, count - k))
        return [value] + [got[k] for k in range(1, count)]

    def swap(value):
        return lax.ppermute(value, "section", [(0, 1), (1, 0)])

    def exchange(part):
        if direct:
            part = call(add_body, out(*part.shape), [part, swap(part)], limit=2 * MIB, name="add")
            return rows_of(part)
        part = lax.psum(part, "section")
        return [lax.all_gather(part, "row", axis=0, tiled=True)]

    own = panel(block)
    if direct:
        kept = rows_of(own)
        kept = kept + [swap(value) for value in kept]
        body = functools.partial(gather_panel_body, count=count, sections=2, tiles=tiles)
        columns = call(body, out(NB * total, LANES), kept, limit=2 * MIB, name="lay")
    else:
        own = jnp.where(lax.axis_index("section") == 0, own, 0.0)
        own = lax.psum(own, "section").reshape(NB, tiles, LANES)
        columns = lax.all_gather(own, "row", axis=1, tiled=True).reshape(NB * total, LANES)
    resident = block

    vector = out(total, LANES)
    facts_shape = out(SUBLANES, LANES)
    part_shape = out(tiles, LANES)
    square = VMEM((LANES, LANES), f32)
    work = 2 * height * breadth

    lefts = []
    rights = []
    left, facts, part = call(
        functools.partial(first_body, breadth=breadth),
        [vector, facts_shape, part_shape],
        [columns, resident],
        scratch=[square],
        flops=work,
        limit=15 * MIB,
        pinned=(1,),
        name="first",
    )
    lefts.append(left)
    offset = None
    base = columns
    for column in range(1, NB):
        pieces = exchange(part)
        args = list(pieces)
        if offset is not None:
            args.append(offset)
        args += [base, lefts[-1], facts, resident]
        right, left, facts, part = call(
            functools.partial(step_body, column=column, count=len(pieces), breadth=breadth),
            [vector, vector, facts_shape, part_shape],
            args,
            scratch=[VMEM((total, LANES), f32), square],
            flops=work,
            limit=15 * MIB,
            pinned=(len(args) - 1,),
            name="step%d" % column,
        )
        rights.append(right)
        outs = [vector, vector] if column + 1 < NB else [vector]
        done = call(
            functools.partial(between_body, column=column),
            outs,
            lefts + rights + [columns, left],
            flops=10**6, limit=2 * MIB,
            name="between%d" % column,
        )
        offset = done[0]
        base = done[-1]
        lefts.append(left)
    pieces = exchange(part)
    slots = 3
    tall = min(256, height)
    operands = list(pieces) + lefts + rights + [offset, facts]
    reduced = pl.pallas_call(
        functools.partial(
            last_body, count=len(pieces), breadth=breadth, slots=slots, tall=tall
        ),
        out_shape=out(height, breadth),
        in_specs=[pl.BlockSpec(memory_space=VMEM)] * (len(operands) + 1),
        out_specs=pl.BlockSpec(memory_space=pl.ANY),
        scratch_shapes=[
            VMEM((total, LANES), f32),
            VMEM((3 * NB * total, LANES), f32),
            VMEM((LANES, breadth), bf16),
            VMEM((tall, LANES), bf16),
            VMEM((slots, tall, breadth), f32),
            pltpu.SemaphoreType.DMA((slots,)),
        ],
        compiler_params=pltpu.CompilerParams(vmem_limit_bytes=15 * MIB),
        cost_estimate=pl.CostEstimate(
            flops=work * 16, bytes_accessed=2 * height * breadth * 4, transcendentals=0
        ),
        name="last",
    )(*operands, pltpu.with_memory_space_constraint(resident, VMEM))
    return reduced.reshape(matrices.shape)


def solution(mesh):
    spec = P("grp", "row", "section")
    return jax.shard_map(local, mesh=mesh, in_specs=(spec,), out_specs=spec, check_vma=False)
```

```python
import functools

import jax
import jax.numpy as jnp
from jax import lax
from jax.experimental import pallas as pl
from jax.experimental.pallas import tpu as pltpu
from jax.sharding import PartitionSpec as P

NB = 8
LANES = 128
SUBLANES = 8
MIB = 1 << 20

VMEM = pltpu.VMEM
f32 = jnp.float32
bf16 = jnp.bfloat16


def call(body, outs, args, scratch=(), flops=0, moved=0, limit=15 * MIB, pinned=(), name=None):
    specs = []
    operands = []
    for index, arg in enumerate(args):
        if index in pinned:
            arg = pltpu.with_memory_space_constraint(arg, VMEM)
        specs.append(pl.BlockSpec(memory_space=VMEM))
        operands.append(arg)
    return pl.pallas_call(
        body,
        out_shape=outs,
        in_specs=specs,
        out_specs=jax.tree.map(lambda _: pl.BlockSpec(memory_space=VMEM), outs),
        scratch_shapes=list(scratch),
        compiler_params=pltpu.CompilerParams(vmem_limit_bytes=limit),
        cost_estimate=pl.CostEstimate(flops=flops, bytes_accessed=moved, transcendentals=0),
        name=name,
    )(*operands)


def out(*shape):
    return jax.ShapeDtypeStruct(shape, f32)


def panel_body(src, dst, tall, sem, *, tiles):
    copy = pltpu.make_async_copy(src.at[:, pl.ds(0, LANES)], tall, sem)
    copy.start()
    copy.wait()
    for t in range(tiles):
        turned = tall[pl.ds(t * LANES, LANES), :].T
        dst[pl.ds(t, NB, stride=tiles), :] = turned[:NB, :]


def panel(block):
    height = block.shape[0]
    tiles = height // LANES
    return pl.pallas_call(
        functools.partial(panel_body, tiles=tiles),
        out_shape=out(NB * tiles, LANES),
        in_specs=[pl.BlockSpec(memory_space=pl.ANY)],
        out_specs=pl.BlockSpec(memory_space=VMEM),
        scratch_shapes=[VMEM((height, LANES), f32), pltpu.SemaphoreType.DMA],
        compiler_params=pltpu.CompilerParams(vmem_limit_bytes=2 * MIB),
        cost_estimate=pl.CostEstimate(flops=10**7, bytes_accessed=2 * MIB, transcendentals=0),
        name="panel",
    )(pltpu.with_memory_space_constraint(block, pltpu.HBM))


def pick_body(own, other, dst):
    dst[...] = jnp.where(lax.axis_index("section") == 0, own[...], other[...])


def gather_panel_body(*refs, tiles):
    *pieces, dst = refs
    total = tiles * len(pieces)
    for piece, place in zip(pieces, ranges_of(len(pieces))):
        for column in range(NB):
            part = pl.multiple_of(column * total + place * tiles, SUBLANES)
            dst[pl.ds(part, tiles), :] = piece[pl.ds(column * tiles, tiles), :]


def ranges_of(count):
    row = lax.axis_index("row")
    if count == 1:
        return [row * 0]
    upper = lax.axis_index("section") == 1
    far = jnp.bitwise_xor(row, 3)
    middle = jnp.bitwise_xor(row, 2)
    return [
        row,
        jnp.bitwise_xor(row, 1),
        jnp.where(upper, far, middle),
        jnp.where(upper, middle, far),
    ]


def total_of(value):
    return jnp.sum(jnp.sum(value, axis=0, keepdims=True), axis=1, keepdims=True)


def place_of(shape):
    return lax.broadcasted_iota(jnp.int32, shape, 0) * LANES + lax.broadcasted_iota(
        jnp.int32, shape, 1
    )


def reflect(current, column):
    place = place_of(current.shape)
    rest = jnp.where(place > column + 1, current, 0.0)
    tail = total_of(rest * rest)
    head = current[0:1, column + 1 : column + 2]
    length = jnp.sqrt(tail + head * head)
    head = head + length
    reflector = jnp.where(place == column + 1, head, rest)
    scaling = 2.0 / (tail + head * head + 1e-06)
    return reflector, scaling, head


def multiply(block, vector, part, wide, *, breadth):
    height = block.shape[0]
    pieces = breadth // LANES
    start = lax.axis_index("section") * pieces
    entries = [vector[pl.ds(start + c, SUBLANES, stride=0), :] for c in range(pieces)]

    def turn(t):
        turned = wide[...].T
        part[pl.ds(t, 1), :] = jnp.sum(turned, axis=0, keepdims=True)

    wide[...] = jnp.zeros_like(wide)

    def step(t, carry):
        turn(jnp.maximum(t - 1, 0))
        for g in range(LANES // SUBLANES):
            rows = pl.ds(pl.multiple_of(t * LANES + g * SUBLANES, SUBLANES), SUBLANES)
            sums = [None, None]
            for c in range(pieces):
                term = block[rows, pl.ds(c * LANES, LANES)] * entries[c]
                sums[c % 2] = term if sums[c % 2] is None else sums[c % 2] + term
            wide[pl.ds(g * SUBLANES, SUBLANES), :] = sums[0] + sums[1]
        return carry

    lax.fori_loop(0, height // LANES, step, 0)
    turn(height // LANES - 1)


def first_body(panel_ref, block, reflector_ref, facts_ref, part, wide, *, breadth):
    rows = reflector_ref.shape[0]
    reflector, scaling, head = reflect(panel_ref[pl.ds(0, rows), :], 0)
    reflector_ref[...] = reflector
    facts_ref[pl.ds(0, 1), :] = jnp.broadcast_to(scaling, (1, LANES))
    facts_ref[pl.ds(1, 1), :] = jnp.broadcast_to(head, (1, LANES))
    multiply(block, reflector_ref, part, wide, breadth=breadth)


def finish_image(pieces, offset, reflector, facts, image_ref):
    for piece, place in zip(pieces, ranges_of(len(pieces))):
        tiles = piece.shape[0]
        place = place * tiles
        image_ref[pl.ds(pl.multiple_of(place, SUBLANES), tiles), :] = piece[...]
    image = image_ref[...]
    if offset is not None:
        image = image - offset[...]
    scaling = facts[0:1, 0:1]
    corrected = scaling * image
    inner = total_of(corrected * reflector)
    return corrected - (0.5 * scaling * inner) * reflector


def step_body(*refs, column, count, breadth):
    pieces = refs[:count]
    refs = refs[count:]
    if column > 1:
        offset, *refs = refs
    else:
        offset = None
    base, old, facts, block, partner_ref, reflector_ref, facts_ref, part, image, wide = refs
    before = old[...]
    partner = finish_image(pieces, offset, before, facts, image)
    partner_ref[...] = partner
    if column == 1:
        base_value = base[pl.ds(old.shape[0], old.shape[0]), :]
    else:
        base_value = base[...]
    current = base_value - before * partner[0:1, column : column + 1] - partner * facts[1:2, 0:1]
    reflector, scaling, head = reflect(current, column)
    reflector_ref[...] = reflector
    facts_ref[pl.ds(0, 1), :] = jnp.broadcast_to(scaling, (1, LANES))
    facts_ref[pl.ds(1, 1), :] = jnp.broadcast_to(head, (1, LANES))
    multiply(block, reflector_ref, part, wide, breadth=breadth)


def between_body(*refs, column):
    lefts = refs[:column]
    rights = refs[column : 2 * column]
    panel_ref, new, offset_ref = refs[2 * column : 2 * column + 3]
    reflector = new[...]
    rows = reflector.shape[0]
    offset = None
    for left, right in zip(lefts, rights):
        left = left[...]
        right = right[...]
        term = left * total_of(right * reflector) + right * total_of(left * reflector)
        offset = term if offset is None else offset + term
    offset_ref[...] = offset
    after = column + 1
    if after < NB:
        base_ref = refs[-1]
        base = panel_ref[pl.ds(after * rows, rows), :]
        for left, right in zip(lefts, rights):
            left = left[...]
            right = right[...]
            base = base - left * right[0:1, after : after + 1]
            base = base - right * left[0:1, after : after + 1]
        base_ref[...] = base


def add_body(a, b, c):
    c[...] = a[...] + b[...]


def split(value):
    high = value.astype(bf16).astype(f32)
    rest = value - high
    middle = rest.astype(bf16).astype(f32)
    low = (rest - middle).astype(bf16).astype(f32)
    return high, middle, low


def last_body(*refs, count, breadth, slots, tall):
    pieces = refs[:count]
    refs = refs[count:]
    lefts = refs[:NB]
    rights = refs[NB : 2 * NB - 1]
    offset, facts, block, dst, image, stack, right_side, left_side, buffer, sems = refs[2 * NB - 1 :]
    total = image.shape[0]
    height = block.shape[0]
    last = lefts[-1][...]
    partner = finish_image(pieces, offset, last, facts, image)
    for k in range(NB):
        stack[pl.ds(k * total, total), :] = lefts[k][...]
        stack[pl.ds((NB + k) * total, total), :] = partner if k == NB - 1 else rights[k][...]
        stack[pl.ds((2 * NB + k) * total, total), :] = lefts[k][...]
    col_start = lax.axis_index("section") * (breadth // LANES)
    row_start = lax.axis_index("row") * (height // LANES)
    pair = 2 * NB

    for c in range(breadth // LANES):
        rows = stack[pl.ds(NB * total + col_start + c, pair, stride=total), :]
        high, middle, low = split(rows)
        group = jnp.concatenate([high, middle, high, middle, low, high, high * 0.0, high * 0.0], 0)
        right_side[:, pl.ds(c * LANES, LANES)] = group.astype(bf16)

    turns = tall // LANES
    steps = height // tall

    def copy_out(step, slot):
        return pltpu.make_async_copy(
            buffer.at[slot], dst.at[pl.ds(pl.multiple_of(step * tall, tall), tall)], sems.at[slot]
        )

    def step(t, carry):
        slot = lax.rem(t, slots)
        for u in range(turns):
            rows = stack[pl.ds(row_start + t * turns + u, pair, stride=total), :]
            high, middle, low = split(rows)
            group = jnp.concatenate(
                [high, high, middle, middle, high, low, high * 0.0, high * 0.0], 0
            )
            left_side[pl.ds(u * LANES, LANES), :] = group.T.astype(bf16)

        @pl.when(t >= slots)
        def _():
            copy_out(t - slots, slot).wait()

        rows = pl.ds(pl.multiple_of(t * tall, tall), tall)
        wide = 512 if breadth % 512 == 0 else LANES
        for c in range(breadth // wide):
            cols = pl.ds(c * wide, wide)
            change = jnp.dot(left_side[...], right_side[:, cols], preferred_element_type=f32)
            buffer[slot, :, cols] = block[rows, cols] - change
        copy_out(t, slot).start()
        return carry

    lax.fori_loop(0, steps, step, 0)
    for t in range(max(0, steps - slots), steps):
        copy_out(t, t % slots).wait()


def local(matrices):
    height, breadth = matrices.shape[1:]
    count = lax.axis_size("row")
    sections = lax.axis_size("section")
    total = count * height // LANES
    tiles = height // LANES
    direct = count == 4 and sections == 2
    block = matrices.reshape(height, breadth)

    def swap(value):
        return lax.ppermute(value, "section", [(0, 1), (1, 0)])

    def rows_of(value):
        near = lax.ppermute(value, "row", [(r, r ^ 1) for r in range(count)])
        apart = [(r, r ^ 2) for r in range(count)]
        apart += [(count + r, count + (r ^ 3)) for r in range(count)]
        first = lax.ppermute(value, ("section", "row"), apart)
        return [value, near, first, swap(first)]

    def exchange(part):
        if direct:
            part = call(add_body, out(*part.shape), [part, swap(part)], limit=2 * MIB, name="add")
            return rows_of(part)
        part = lax.psum(part, "section")
        return [lax.all_gather(part, "row", axis=0, tiled=True)]

    own = panel(block)
    if direct:
        own = call(pick_body, out(*own.shape), [own, swap(own)], limit=2 * MIB, name="pick")
        body = functools.partial(gather_panel_body, tiles=tiles)
        columns = call(body, out(NB * total, LANES), rows_of(own), limit=2 * MIB, name="lay")
    else:
        own = jnp.where(lax.axis_index("section") == 0, own, 0.0)
        own = lax.psum(own, "section").reshape(NB, tiles, LANES)
        columns = lax.all_gather(own, "row", axis=1, tiled=True).reshape(NB * total, LANES)
    resident = block

    vector = out(total, LANES)
    facts_shape = out(SUBLANES, LANES)
    part_shape = out(tiles, LANES)
    square = VMEM((LANES, LANES), f32)
    work = 2 * height * breadth

    lefts = []
    rights = []
    left, facts, part = call(
        functools.partial(first_body, breadth=breadth),
        [vector, facts_shape, part_shape],
        [columns, resident],
        scratch=[square],
        flops=work,
        limit=15 * MIB,
        pinned=(1,),
        name="first",
    )
    lefts.append(left)
    offset = None
    base = columns
    for column in range(1, NB):
        pieces = exchange(part)
        args = list(pieces)
        if offset is not None:
            args.append(offset)
        args += [base, lefts[-1], facts, resident]
        right, left, facts, part = call(
            functools.partial(step_body, column=column, count=len(pieces), breadth=breadth),
            [vector, vector, facts_shape, part_shape],
            args,
            scratch=[VMEM((total, LANES), f32), square],
            flops=work,
            limit=15 * MIB,
            pinned=(len(args) - 1,),
            name="step%d" % column,
        )
        rights.append(right)
        outs = [vector, vector] if column + 1 < NB else [vector]
        done = call(
            functools.partial(between_body, column=column),
            outs,
            lefts + rights + [columns, left],
            flops=10**6, limit=2 * MIB,
            name="between%d" % column,
        )
        offset = done[0]
        base = done[-1]
        lefts.append(left)
    pieces = exchange(part)
    slots = 3
    tall = min(256, height)
    operands = list(pieces) + lefts + rights + [offset, facts]
    reduced = pl.pallas_call(
        functools.partial(
            last_body, count=len(pieces), breadth=breadth, slots=slots, tall=tall
        ),
        out_shape=out(height, breadth),
        in_specs=[pl.BlockSpec(memory_space=VMEM)] * (len(operands) + 1),
        out_specs=pl.BlockSpec(memory_space=pl.ANY),
        scratch_shapes=[
            VMEM((total, LANES), f32),
            VMEM((3 * NB * total, LANES), f32),
            VMEM((LANES, breadth), bf16),
            VMEM((tall, LANES), bf16),
            VMEM((slots, tall, breadth), f32),
            pltpu.SemaphoreType.DMA((slots,)),
        ],
        compiler_params=pltpu.CompilerParams(vmem_limit_bytes=15 * MIB),
        cost_estimate=pl.CostEstimate(
            flops=work * 16, bytes_accessed=2 * height * breadth * 4, transcendentals=0
        ),
        name="last",
    )(*operands, pltpu.with_memory_space_constraint(resident, VMEM))
    return reduced.reshape(matrices.shape)


def solution(mesh):
    spec = P("grp", "row", "section")
    return jax.shard_map(local, mesh=mesh, in_specs=(spec,), out_specs=spec, check_vma=False)
```
